32 devices in a mesh: samp: 4 (over z), seq: 8 (over y, x, core).
Axes of the slice: x: 2, y: 2, z: 4, core: 2. Of those that a mesh axis runs over, the one named last changes fastest.
Arguments:
- queries: bfloat16 [4, 4096, 3584], P('samp', 'seq'), may hold values from -200 to 200
- keys: bfloat16 [4, 4096, 512], P('samp', 'seq'), may hold values from -6 to 6
- values: bfloat16 [4, 4096, 512], P('samp', 'seq'), may hold values from -6 to 6
- reg_owner: int32 [4], P('samp'), may hold values from 0 to 7
- block_lists: int32 [4, 32, 8], P('samp', 'seq'), may hold values from 0 to 31, as said below
- list_counts: int32 [4, 32], P('samp', 'seq'), may hold values from 0 to 8, as said below
- image_blocks: int32 [4, 32], P('samp', 'seq'), may hold values from 0 to 1, as said below
Outputs:
- attended: bfloat16 [4, 4096, 3584], P('samp', 'seq')
The draws below stay inside these ranges and needn't reach their ends.
Inputs may be any that keep to these rules, and one draw needn't show every extreme that they name: `block_lists`: block b lies on sequence index b // 4. Entry t of a list is used only where t < the block's count, unused entries are 0. The used entries of one block name blocks of distinct sequence indices other than its own. Over all blocks of one sequence index, at most one distinct block of each other sequence index is named. On the last sequence index of each sample, the lists together name a block of every other index. `list_counts`: 0 for image blocks; at most 8. `image_blocks`: the blocks of the last sequence index of each sample are text blocks.
All inputs are finite; a program needn't handle non-finite values.
Results may differ from the reference program's by a relative error of at most 0.0043.
Values may be sent and summed in bfloat16 or wider, within the bound.
No kernel may reach another device: no remote copies, remote signals or barrier semaphores. Data moves between devices by JAX's collectives and lax.ppermute only.
A program may use at most 128 MiB of HBM per device.

```python
import math
import jax
import jax.numpy as jnp
from jax import lax

QUERY_HEADS = 28
KEY_VALUE_HEADS = 4
HEAD_SIZE = 128
BLOCK_TOKENS = 128
REG = 64
LIST_ENTRIES = 8
BLK_DEV = 4
SAMPLE_COUNT = 4
TOK_DEV = 512
SAMPLE_BLOCKS = 32
SAMPLE_TOKENS = 4096
N_SEQ = 8


def activations(key):
    seeded = jax.random.fold_in(key, 11)
    key_queries, keys_for_keys = jax.random.split(seeded, 2)
    key_region = jnp.clip(jax.random.normal(keys_for_keys, (SAMPLE_COUNT, SAMPLE_TOKENS, KEY_VALUE_HEADS, HEAD_SIZE), jnp.float32), -6.0, 6.0)
    query_field = jnp.clip(jax.random.normal(key_queries, (SAMPLE_COUNT, SAMPLE_TOKENS, QUERY_HEADS, HEAD_SIZE), jnp.float32), -6.0, 6.0)
    query_out = query_field.reshape(SAMPLE_COUNT, SAMPLE_TOKENS, QUERY_HEADS * HEAD_SIZE).astype(jnp.bfloat16)
    key_output = key_region.reshape(SAMPLE_COUNT, SAMPLE_TOKENS, KEY_VALUE_HEADS * HEAD_SIZE).astype(jnp.bfloat16)
    return (query_out, key_output)


def draw_queries(key, part):
    return activations(key)[0]


def draw_keys(key, part):
    return activations(key)[1]


def layout(key):
    seeded = jax.random.fold_in(key, 7)
    key_kinds, key_chosen, key_order, key_counts = jax.random.split(seeded, 4)
    block_ids = jnp.arange(SAMPLE_BLOCKS, dtype=jnp.int32)
    block_device = block_ids // BLK_DEV
    local_ids = block_ids % BLK_DEV
    last_device = N_SEQ - 1
    kinds = (jax.random.randint(key_kinds, (SAMPLE_COUNT, SAMPLE_BLOCKS), 0, 4, jnp.int32) == 0).astype(jnp.int32)
    kinds = jnp.where(block_device[None, :] == last_device, 0, kinds)
    chosen = jax.random.randint(key_chosen, (SAMPLE_COUNT, N_SEQ, N_SEQ), 0, BLK_DEV, jnp.int32)
    owner_ids = jnp.arange(N_SEQ, dtype=jnp.int32)
    ranking = jax.random.randint(key_order, (SAMPLE_COUNT, SAMPLE_BLOCKS, N_SEQ), 0, 2 ** 16, jnp.int32) * N_SEQ + owner_ids
    ranking = jnp.where(owner_ids[None, None, :] != block_device[None, :, None], ranking, 2 ** 30)
    ordered = jnp.argsort(ranking, axis=-1)[..., :LIST_ENTRIES].astype(jnp.int32)
    slot_ids = jnp.arange(LIST_ENTRIES, dtype=jnp.int32)
    full_count = min(LIST_ENTRIES, N_SEQ - 1)
    cyclic = (local_ids[:, None] * full_count + slot_ids[None, :]) % (N_SEQ - 1)
    is_last = block_device == last_device
    ordered = jnp.where(is_last[None, :, None], cyclic[None], ordered)
    counts = full_count - jax.random.randint(key_counts, (SAMPLE_COUNT, SAMPLE_BLOCKS), 0, 3, jnp.int32)
    counts = jnp.where(is_last[None, :], full_count, counts)
    counts = jnp.where(kinds == 1, 0, counts)
    chosen_rows = chosen[:, block_device, :]
    picked = jnp.take_along_axis(chosen_rows, ordered, axis=2)
    list_ids = ordered * BLK_DEV + picked
    list_ids = jnp.where(slot_ids[None, None, :] < counts[..., None], list_ids, 0)
    return (list_ids.astype(jnp.int32), counts.astype(jnp.int32), kinds.astype(jnp.int32))


def draw_block_lists(key, part):
    return layout(key)[0]


def draw_list_counts(key, part):
    return layout(key)[1]


def draw_image_blocks(key, part):
    return layout(key)[2]


def place_ends(result, key, smallest, high):
    index_at = [jax.random.randint(jax.random.fold_in(key, axis), (), 0, length) for axis, length in enumerate(result.shape)]
    widest = result.shape.index(max(result.shape))
    beside = index_at[:widest] + [(index_at[widest] + 1) % result.shape[widest]] + index_at[widest + 1:]
    return result.at[tuple(index_at)].set(smallest).at[tuple(beside)].set(high)


def shard_levels(own_key, shape, cuts, low, high):
    gain = 1.0
    for dim, blocks in cuts:
        heights = jax.random.uniform(jax.random.fold_in(jax.random.fold_in(own_key, 6), dim), (blocks,), jnp.float32, low / len(cuts), high / len(cuts))
        gain = gain * jnp.repeat(jnp.exp(heights), shape[dim] // blocks).reshape((-1,) + (1,) * (len(shape) - 1 - dim))
    return gain


def normal_values(key, extent, width, most, pieces=(), kind=jnp.bfloat16):
    drawn = width * jax.random.normal(key, extent, jnp.float32)
    if pieces:
        drawn = drawn * shard_levels(key, extent, pieces, -0.22, 0.18)
    return jnp.clip(drawn, -most, most).astype(kind)


def setup_inputs(seed: int = 0) -> dict:
    splits = jax.random.split(jax.random.key(seed), 8)
    return {
        "queries": draw_queries(jax.random.fold_in(splits[7], 71), 0),
        "keys": draw_keys(jax.random.fold_in(splits[7], 71), 0),
        "values": normal_values(splits[2], (SAMPLE_COUNT, SAMPLE_TOKENS, KEY_VALUE_HEADS * HEAD_SIZE), 1.0, 6.0, ((0, 4), (1, 8))),
        "reg_owner": place_ends(jax.random.randint(splits[3], (SAMPLE_COUNT,), 0, N_SEQ), jax.random.fold_in(splits[3], 1), 0, N_SEQ - 1).astype(jnp.int32),
        "block_lists": draw_block_lists(jax.random.fold_in(splits[7], 71), 0),
        "list_counts": draw_list_counts(jax.random.fold_in(splits[7], 71), 0),
        "image_blocks": draw_image_blocks(jax.random.fold_in(splits[7], 71), 0),
    }


very_low = -1e+30

def group_part(query_row_list, key_row_list, value_row_list, visible):
    head_grouped = query_row_list.astype(jnp.float32).reshape(BLOCK_TOKENS, KEY_VALUE_HEADS, QUERY_HEADS // KEY_VALUE_HEADS, HEAD_SIZE)
    per_head_keys = key_row_list.astype(jnp.float32).reshape(-1, KEY_VALUE_HEADS, HEAD_SIZE)
    per_head_values = value_row_list.astype(jnp.float32).reshape(-1, KEY_VALUE_HEADS, HEAD_SIZE)
    scores = jnp.einsum('qhgd,khd->hgqk', head_grouped, per_head_keys) / math.sqrt(HEAD_SIZE)
    scores = jnp.where(visible, scores, very_low)
    maxima = lax.optimization_barrier(jnp.max(scores, axis=-1))
    weights = jnp.where(visible, jnp.exp(scores - maxima[..., None]), 0.0)
    totals = lax.optimization_barrier(jnp.sum(weights, axis=-1))
    rounded = lax.optimization_barrier(weights.astype(jnp.bfloat16)).astype(jnp.float32)
    partial_value = jnp.einsum('hgqk,khd->hgqd', rounded, per_head_values)
    return (maxima, totals, partial_value)

def combine(parts):
    top_score = jnp.maximum(jnp.maximum(parts[0][0], parts[1][0]), parts[2][0])
    numerator = jnp.zeros(parts[0][2].shape, jnp.float32)
    denominator = jnp.zeros(parts[0][1].shape, jnp.float32)
    for maxima, totals, partial_value in parts:
        rescale = jnp.exp(maxima - top_score)
        numerator = numerator + rescale[..., None] * partial_value
        denominator = denominator + rescale * totals
    merged = numerator / denominator[..., None]
    return merged.transpose(2, 0, 1, 3).reshape(merged.shape[2], -1)

def reference(queries, keys, values, reg_owner, block_lists, list_counts, image_blocks):
    outputs = []
    row_ids = jnp.arange(BLOCK_TOKENS)
    slot_rows = jnp.arange(LIST_ENTRIES * BLOCK_TOKENS) // BLOCK_TOKENS
    for sample in range(SAMPLE_COUNT):
        query_all = queries[sample]
        every_key = keys[sample]
        every_value = values[sample]
        blocked_keys = every_key.reshape(SAMPLE_BLOCKS, BLOCK_TOKENS, KEY_VALUE_HEADS * HEAD_SIZE)
        blocked_values = every_value.reshape(SAMPLE_BLOCKS, BLOCK_TOKENS, KEY_VALUE_HEADS * HEAD_SIZE)
        reg_start = (reg_owner[sample] * TOK_DEV).astype(jnp.int32)
        reg_keys = lax.dynamic_slice_in_dim(every_key, reg_start, REG, 0)
        reg_values = lax.dynamic_slice_in_dim(every_value, reg_start, REG, 0)
        sample_lists = block_lists[sample]
        sample_counts = list_counts[sample]
        sample_image = image_blocks[sample]

        def one_block(block_id):
            row_start = (block_id * BLOCK_TOKENS).astype(jnp.int32)
            query_row_list = lax.dynamic_slice_in_dim(query_all, row_start, BLOCK_TOKENS, 0)
            own_keys = lax.dynamic_slice_in_dim(every_key, row_start, BLOCK_TOKENS, 0)
            own_values = lax.dynamic_slice_in_dim(every_value, row_start, BLOCK_TOKENS, 0)
            listed_block_index = sample_lists[block_id]
            remote_keys = blocked_keys[listed_block_index].reshape(LIST_ENTRIES * BLOCK_TOKENS, KEY_VALUE_HEADS * HEAD_SIZE)
            remote_values = blocked_values[listed_block_index].reshape(LIST_ENTRIES * BLOCK_TOKENS, KEY_VALUE_HEADS * HEAD_SIZE)
            reg_visible = jnp.ones((BLOCK_TOKENS, REG), bool)
            own_visible = (row_ids[None, :] <= row_ids[:, None]) | (sample_image[block_id] == 1)
            far_visible = jnp.broadcast_to(slot_rows[None, :] < sample_counts[block_id], (BLOCK_TOKENS, LIST_ENTRIES * BLOCK_TOKENS))
            parts = [group_part(query_row_list, reg_keys, reg_values, reg_visible), group_part(query_row_list, own_keys, own_values, own_visible), group_part(query_row_list, remote_keys, remote_values, far_visible)]
            return combine(parts).astype(jnp.bfloat16)
        blocks_out = lax.map(one_block, jnp.arange(SAMPLE_BLOCKS, dtype=jnp.int32))
        outputs.append(blocks_out.reshape(SAMPLE_TOKENS, QUERY_HEADS * HEAD_SIZE))
    return jnp.stack(outputs)
```

```python
import functools
import math

import jax
import jax.numpy as jnp
from jax import lax
from jax.experimental import pallas as pl
from jax.experimental.pallas import tpu as pltpu
from jax.sharding import PartitionSpec as P

QUERY_HEADS = 28
KEY_VALUE_HEADS = 4
HEAD_SIZE = 128
REG = 64
GROUP = QUERY_HEADS // KEY_VALUE_HEADS
ONES_ROWS = 16
CHUNKS = ((0, 2), (2, 1), (3, 1))
SCORE_SCALE = math.log2(math.e) / math.sqrt(HEAD_SIZE)
NT = (((1,), (1,)), ((), ()))
NN = (((1,), (0,)), ((), ()))


def select_kernel(chips, rows, me_ref, *refs):
    tables = refs[: chips - 1]
    own_k, own_v, mate_k, mate_v = refs[chips - 1 : chips + 3]
    sends = refs[chips + 3 :]
    me = me_ref[0]
    mate = me ^ 1
    for chip in range(chips - 1):
        for side, (keys, values, who) in enumerate(
            ((own_k, own_v, me), (mate_k, mate_v, mate))
        ):
            start = pl.multiple_of(tables[chip][who] * rows, rows)
            for piece, (first, count) in enumerate(CHUNKS):
                out = sends[piece * (chips - 1) + chip]
                cols = slice(first * HEAD_SIZE, (first + count) * HEAD_SIZE)
                out[side, 0] = keys[pl.ds(start, rows), cols]
                out[side, 1] = values[pl.ds(start, rows), cols]


def select_blocks(me, tables, own_k, own_v, mate_k, mate_v, rows):
    chips = len(tables) + 1
    smem = pl.BlockSpec(memory_space=pltpu.SMEM)
    vmem = pl.BlockSpec(memory_space=pltpu.VMEM)
    shapes = [
        jax.ShapeDtypeStruct((2, 2, rows, count * HEAD_SIZE), jnp.bfloat16)
        for _, count in CHUNKS
        for _ in range(chips - 1)
    ]
    return pl.pallas_call(
        functools.partial(select_kernel, chips, rows),
        in_specs=[smem] * chips + [vmem] * 4,
        out_specs=[vmem] * len(shapes),
        out_shape=shapes,
        name="select_blocks",
    )(me, *tables, own_k, own_v, mate_k, mate_v)


def attend_kernel(received, slots, rows, reg, table, image, mate_block, *refs):
    q_ref, own_k, own_v, mate_k, mate_v = refs[:5]
    arrived = refs[5 : 5 + received]
    reg_k, reg_v, _, out_ref = refs[5 + received : 9 + received]
    key_pool, value_pool, reg_value, s0, s1, p0, p1 = refs[9 + received :]
    score_refs = (s0, s1)
    weight_refs = (p0, p1)
    blocks = own_k.shape[0] // rows
    fill = key_pool.shape[0] - 1
    row_ids = lax.broadcasted_iota(jnp.int32, (ONES_ROWS, rows), 0)
    ones = jnp.where(row_ids == 0, 1.0, 0.0).astype(jnp.bfloat16)

    def put(slot, keys, values):
        key_pool[slot] = keys
        value_pool[slot, :HEAD_SIZE] = values.T
        value_pool[slot, HEAD_SIZE:] = ones

    for b in range(blocks):
        put(b, own_k[b * rows : (b + 1) * rows], own_v[b * rows : (b + 1) * rows])
    start = pl.multiple_of(mate_block[0] * rows, rows)
    put(blocks, mate_k[pl.ds(start, rows)], mate_v[pl.ds(start, rows)])
    for d in range(received):
        for side in range(2):
            put(blocks + 1 + 2 * d + side, arrived[d][side, 0], arrived[d][side, 1])
    for r in range(rows // reg):
        key_pool[fill, r * reg : (r + 1) * reg] = reg_k[...]
    value_pool[fill] = jnp.zeros(value_pool.shape[1:], jnp.bfloat16)
    reg_value[:HEAD_SIZE] = reg_v[...].T
    reg_value[HEAD_SIZE:] = ones[:, :reg]

    steps = [
        (b, 2 * j, min(2 * j + 2, GROUP)) for b in range(blocks) for j in range((GROUP + 1) // 2)
    ]
    tops = {}

    def scores(i):
        b, lo, hi = steps[i]
        wide = (hi - lo) * rows
        out = score_refs[i % 2]
        keys = jnp.concatenate(
            [key_pool[b]] + [key_pool[table[b, t]] for t in range(slots)] + [reg_k[...]], axis=0
        )
        q = jnp.concatenate(
            [
                q_ref[b * rows : (b + 1) * rows, c * HEAD_SIZE : (c + 1) * HEAD_SIZE]
                for c in range(lo, hi)
            ],
            axis=0,
        )
        s = lax.dot_general(keys, q, NT, preferred_element_type=jnp.float32)
        key_row = lax.broadcasted_iota(jnp.int32, (rows, wide), 0)
        query_row = lax.broadcasted_iota(jnp.int32, (rows, wide), 1) % rows
        own = jnp.where((key_row <= query_row) | (image[b] == 1), s[:rows], -jnp.inf)
        top = jnp.maximum(
            jnp.max(own, axis=0, keepdims=True), jnp.max(s[rows:], axis=0, keepdims=True)
        )
        tops[i] = top * SCORE_SCALE
        out[:rows, :wide] = own
        out[rows:, :wide] = s[rows:]

    def weights(i):
        b, lo, hi = steps[i]
        wide = (hi - lo) * rows
        s = score_refs[i % 2]
        p = jnp.exp2(s[:, :wide] * SCORE_SCALE - tops.pop(i))
        weight_refs[i % 2][:, :wide] = p.astype(jnp.bfloat16)

    def output(i):
        b, lo, hi = steps[i]
        wide = (hi - lo) * rows
        values = jnp.concatenate(
            [value_pool[b]] + [value_pool[table[b, t]] for t in range(slots)] + [reg_value[...]],
            axis=1,
        )
        o = lax.dot_general(
            values, weight_refs[i % 2][:, :wide], NN, preferred_element_type=jnp.float32
        )
        o = o[:HEAD_SIZE] * (1.0 / o[HEAD_SIZE : HEAD_SIZE + 1])
        for c in range(lo, hi):
            out_ref[b * rows : (b + 1) * rows, c * HEAD_SIZE : (c + 1) * HEAD_SIZE] = (
                o[:, (c - lo) * rows : (c - lo + 1) * rows].T.astype(jnp.bfloat16)
            )

    count = len(steps)
    for i in range(count + 2):
        if i < count:
            scores(i)
        if 0 <= i - 1 < count:
            weights(i - 1)
        if 0 <= i - 2 < count:
            output(i - 2)


def attend(table, image, mate_block, q, own_k, own_v, mate_k, mate_v, arrived, regs, out, chunk):
    first, heads = chunk
    tokens = q.shape[0]
    blocks, slots = table.shape
    rows = tokens // blocks
    reg = regs[0].shape[0]
    pool = blocks + 2 + 2 * len(arrived)
    keys = rows * (1 + slots) + reg
    smem = pl.BlockSpec(memory_space=pltpu.SMEM)

    def column(height):
        return pl.BlockSpec((height, HEAD_SIZE), lambda h: (0, first + h))

    wide = pl.BlockSpec((tokens, GROUP * HEAD_SIZE), lambda h: (0, first + h))
    block = pl.BlockSpec((2, 2, rows, HEAD_SIZE), lambda h: (0, 0, 0, h))
    operands = [table, image, mate_block, q, own_k, own_v, mate_k, mate_v, *arrived, *regs]
    specs = [smem] * 3 + [wide] + [column(tokens)] * 4 + [block] * len(arrived) + [column(reg)] * 2
    aliases = {}
    if out is None:
        out = jnp.zeros((8, 128), jnp.bfloat16)
    else:
        aliases = {len(operands): 0}
    operands.append(out)
    specs.append(pl.BlockSpec(memory_space=pl.ANY))
    return pl.pallas_call(
        functools.partial(attend_kernel, len(arrived), slots, rows, reg),
        grid=(heads,),
        in_specs=specs,
        out_specs=wide,
        out_shape=jax.ShapeDtypeStruct(q.shape, jnp.bfloat16),
        scratch_shapes=[
            pltpu.VMEM((pool, rows, HEAD_SIZE), jnp.bfloat16),
            pltpu.VMEM((pool, HEAD_SIZE + ONES_ROWS, rows), jnp.bfloat16),
            pltpu.VMEM((HEAD_SIZE + ONES_ROWS, reg), jnp.bfloat16),
            pltpu.VMEM((keys, 2 * rows), jnp.float32),
            pltpu.VMEM((keys, 2 * rows), jnp.float32),
            pltpu.VMEM((keys, 2 * rows), jnp.bfloat16),
            pltpu.VMEM((keys, 2 * rows), jnp.bfloat16),
        ],
        input_output_aliases=aliases,
        cost_estimate=pl.CostEstimate(
            flops=4 * heads * GROUP * tokens * keys * HEAD_SIZE,
            bytes_accessed=4 * heads * GROUP * tokens * HEAD_SIZE,
            transcendentals=heads * GROUP * tokens * keys,
        ),
        name=f"attend_{first}",
    )(*operands)


def per_device(queries, keys, values, reg_owner, block_lists, list_counts, image_blocks):
    q = queries[0]
    own_k = keys[0]
    own_v = values[0]
    lists = block_lists[0]
    counts = list_counts[0]
    devices = lax.axis_size("seq")
    chips = devices // 2
    me = lax.axis_index("seq")
    mate = me ^ 1
    blocks = lists.shape[0]
    slots = min(lists.shape[1], devices - 1)
    rows = own_k.shape[0] // blocks

    def swap(x, offset):
        return lax.ppermute(x, "seq", [(i, i ^ offset) for i in range(devices)])

    lists = lists[:, :slots]
    live = jnp.arange(slots, dtype=jnp.int32)[None, :] < counts[:, None]
    owner = lists // blocks
    named = live[:, :, None] & (owner[:, :, None] == jnp.arange(devices, dtype=jnp.int32))
    wanted = jnp.max(jnp.where(named, (lists % blocks)[:, :, None], 0), axis=(0, 1))
    tables = [swap(wanted, 2 * d) for d in range(1, chips)]
    mate_k = swap(own_k, 1)
    mate_v = swap(own_v, 1)

    sends = select_blocks(
        me.reshape(1), tables, own_k, own_v, mate_k, mate_v, rows
    )
    arrived = [
        [swap(sends[piece * (chips - 1) + d - 1], 2 * d) for d in range(1, chips)]
        for piece in range(len(CHUNKS))
    ]

    root = reg_owner[0]
    low = me % 2 == 0
    at_mate = (root ^ me) % 2 == 1
    half = jnp.where(
        low,
        jnp.where(at_mate, mate_k[:REG], own_k[:REG]),
        jnp.where(at_mate, mate_v[:REG], own_v[:REG]),
    )
    bit = 2
    while bit < devices:
        half = jnp.where(((root ^ me) & bit) != 0, swap(half, bit), half)
        bit *= 2
    other = swap(half, 1)
    regs = (jnp.where(low, half, other), jnp.where(low, other, half))

    fill = blocks + devices - 1
    table = jnp.where(live, blocks - 1 + (owner ^ me), fill)
    mate_block = jnp.sum(jnp.where(jnp.arange(devices) == mate, wanted, 0)).reshape(1)
    out = None
    for piece, chunk in enumerate(CHUNKS):
        out = attend(
            table,
            image_blocks[0],
            mate_block,
            q,
            own_k,
            own_v,
            mate_k,
            mate_v,
            arrived[piece],
            regs,
            out,
            chunk,
        )
    return out[None]


def solution(mesh):
    placed = (
        P("samp", "seq", None),
        P("samp", "seq", None),
        P("samp", "seq", None),
        P("samp"),
        P("samp", "seq", None),
        P("samp", "seq"),
        P("samp", "seq"),
    )
    return jax.shard_map(
        per_device, mesh=mesh, in_specs=placed, out_specs=P("samp", "seq", None), check_vma=False
    )
```

```python
import functools
import math

import jax
import jax.numpy as jnp
from jax import lax
from jax.experimental import pallas as pl
from jax.experimental.pallas import tpu as pltpu
from jax.sharding import PartitionSpec as P


QUERY_HEADS = 28
KEY_VALUE_HEADS = 4
HEAD_SIZE = 128
REG = 64
GROUP = QUERY_HEADS // KEY_VALUE_HEADS
ONES_ROWS = 16
CHUNKS = ((0, 2), (2, 2))
SELECT_VMEM = int(56 * 2**20)
ATTEND_VMEM = int(56 * 2**20)
SCORE_SCALE = math.log2(math.e) / math.sqrt(HEAD_SIZE)
LARGEST_POWER = 64.0
NT = (((1,), (1,)), ((), ()))
NN = (((1,), (0,)), ((), ()))


def select_kernel(chips, rows, me_ref, *refs):
    tables = refs[: chips - 1]
    own_k, own_v, mate_k, mate_v = refs[chips - 1 : chips + 3]
    sends = refs[chips + 3 : -3]
    held, read_sem, write_sem = refs[-3:]
    me = me_ref[0]
    blocks = own_k.shape[0] // rows
    reads = []
    for chip in range(chips - 1):
        table = tables[chip]
        for side, (keys, values) in enumerate(((own_k, own_v), (mate_k, mate_v))):
            base = (me ^ side) * blocks
            block = jnp.int32(0)
            for b in range(table.shape[0]):
                for t in range(table.shape[1]):
                    place = table[b, t] - base
                    block = jnp.where((place >= 0) & (place < blocks), place, block)
            start = pl.multiple_of(block * rows, rows)
            for i, source in enumerate((keys, values)):
                copy = pltpu.make_async_copy(
                    source.at[pl.ds(start, rows)],
                    held.at[chip, side, i],
                    read_sem.at[chip, side, i],
                )
                copy.start()
                reads.append(copy)
    writes = []
    for chip in range(chips - 1):
        for copy in reads[4 * chip : 4 * chip + 4]:
            copy.wait()
        for piece, (first, count) in enumerate(CHUNKS):
            cols = pl.ds(first * HEAD_SIZE, count * HEAD_SIZE)
            copy = pltpu.make_async_copy(
                held.at[chip, :, :, :, cols],
                sends[piece * (chips - 1) + chip],
                write_sem.at[piece, chip],
            )
            copy.start()
            writes.append(copy)
    for copy in writes:
        copy.wait()


def select_blocks(me, tables, own_k, own_v, mate_k, mate_v, rows):
    chips = len(tables) + 1
    smem = pl.BlockSpec(memory_space=pltpu.SMEM)
    anywhere = pl.BlockSpec(memory_space=pl.ANY)
    shapes = [
        jax.ShapeDtypeStruct((2, 2, rows, count * HEAD_SIZE), jnp.bfloat16)
        for _, count in CHUNKS
        for _ in range(chips - 1)
    ]
    return pl.pallas_call(
        functools.partial(select_kernel, chips, rows),
        in_specs=[smem] * chips + [anywhere] * 4,
        out_specs=[anywhere] * len(shapes),
        out_shape=shapes,
        scratch_shapes=[
            pltpu.VMEM((chips - 1, 2, 2, rows, own_k.shape[1]), jnp.bfloat16),
            pltpu.SemaphoreType.DMA((chips - 1, 2, 2)),
            pltpu.SemaphoreType.DMA((len(CHUNKS), chips - 1)),
        ],
        compiler_params=pltpu.CompilerParams(vmem_limit_bytes=SELECT_VMEM),
        name="select_blocks",
    )(me, *tables, own_k, own_v, mate_k, mate_v)


def attend_kernel(first, received, slots, rows, reg, listed, image, me_ref, *refs):
    q_ref, own_k, own_v, mate_k, mate_v = refs[:5]
    arrived = refs[5 : 5 + received]
    reg_k, reg_v = refs[5 + received : 7 + received]
    refs = refs[7 + received :]
    if first > 0:
        refs = refs[1:]
    out_ref = refs[0]
    key_pool, value_pool, reg_value, p0, p1, q_buf, k_buf, v_buf, sem = refs[1:]
    step = pl.program_id(0)
    heads = pl.num_programs(0)

    def fetch(h):
        slot = h % 2
        own = pl.ds(pl.multiple_of((first + h) * HEAD_SIZE, HEAD_SIZE), HEAD_SIZE)
        width = GROUP * HEAD_SIZE
        wide = pl.ds(pl.multiple_of((first + h) * width, HEAD_SIZE), width)
        return (
            pltpu.make_async_copy(q_ref.at[:, wide], q_buf.at[slot], sem.at[0, slot]),
            pltpu.make_async_copy(own_k.at[:, own], k_buf.at[slot], sem.at[1, slot]),
            pltpu.make_async_copy(own_v.at[:, own], v_buf.at[slot], sem.at[2, slot]),
        )

    @pl.when(step == 0)
    def _():
        for copy in fetch(0):
            copy.start()

    @pl.when(step + 1 < heads)
    def _():
        for copy in fetch(step + 1):
            copy.start()

    waits = fetch(step)
    q_ref = q_buf.at[step % 2]
    keys_ref = k_buf.at[step % 2]
    values_ref = v_buf.at[step % 2]
    weight_refs = (p0, p1)
    blocks = own_k.shape[0] // rows
    fill = key_pool.shape[0] - 1
    row_ids = lax.broadcasted_iota(jnp.int32, (ONES_ROWS, rows), 0)
    ones = jnp.where(row_ids == 0, 1.0, 0.0).astype(jnp.bfloat16)

    @pl.when(step == 0)
    def _():
        for slot in range(fill):
            value_pool[slot, HEAD_SIZE:] = ones
        value_pool[fill] = jnp.zeros(value_pool.shape[1:], jnp.bfloat16)
        reg_value[HEAD_SIZE:] = ones[:, :reg]

    def put(slot, keys, values):
        key_pool[slot] = keys
        value_pool[slot, :HEAD_SIZE] = values.T

    for copy in waits:
        copy.wait()
    for b in range(blocks):
        put(b, keys_ref[b * rows : (b + 1) * rows], values_ref[b * rows : (b + 1) * rows])
    me = me_ref[0]
    table = {}
    from_mate = jnp.int32(0)
    for b in range(blocks):
        for t in range(slots):
            entry = listed[b, t]
            away = (entry // blocks) ^ me
            table[b, t] = jnp.where(entry >= 0, blocks - 1 + away, fill)
            from_mate = jnp.where((entry >= 0) & (away == 1), entry % blocks, from_mate)
    start = pl.multiple_of(from_mate * rows, rows)
    put(blocks, mate_k[pl.ds(start, rows)], mate_v[pl.ds(start, rows)])
    for d in range(received):
        for side in range(2):
            put(blocks + 1 + 2 * d + side, arrived[d][side, 0], arrived[d][side, 1])
    for r in range(rows // reg):
        key_pool[fill, r * reg : (r + 1) * reg] = reg_k[...]
    reg_value[:HEAD_SIZE] = reg_v[...].T

    steps = [
        (b, 2 * j, min(2 * j + 2, GROUP)) for b in range(blocks) for j in range((GROUP + 1) // 2)
    ]
    over = []

    def causal(b, wide):
        key_row = lax.broadcasted_iota(jnp.int32, (rows, wide), 0)
        query_row = lax.broadcasted_iota(jnp.int32, (rows, wide), 1) % rows
        return (key_row <= query_row) | (image[b] == 1)

    def weights(i):
        b, lo, hi = steps[i]
        wide = (hi - lo) * rows
        p_ref = weight_refs[i % 2]
        q = jnp.concatenate(
            [
                q_ref[b * rows : (b + 1) * rows, c * HEAD_SIZE : (c + 1) * HEAD_SIZE]
                for c in range(lo, hi)
            ],
            axis=0,
        )
        near_keys = jnp.concatenate([key_pool[b], reg_k[...]], axis=0)
        far_keys = jnp.concatenate([key_pool[table[b, t]] for t in range(slots)], axis=0)
        near = lax.dot_general(near_keys, q, NT, preferred_element_type=jnp.float32)
        far = lax.dot_general(far_keys, q, NT, preferred_element_type=jnp.float32)
        own = jnp.where(causal(b, wide), near[:rows], -jnp.inf)
        base = jnp.maximum(
            jnp.max(own, axis=0, keepdims=True), jnp.max(near[rows:], axis=0, keepdims=True)
        )
        top = jnp.max(far.reshape(-1, 8, wide), axis=0) - base
        over.append(jnp.maximum(top[:, :rows], top[:, wide - rows :]))

        def weigh(s):
            return jnp.exp2((s - base) * SCORE_SCALE).astype(jnp.bfloat16)

        p_ref[:rows, :wide] = weigh(own)
        p_ref[rows : -reg, :wide] = weigh(far)
        p_ref[-reg:, :wide] = weigh(near[rows:])

    def gather_values(b, slot):
        return jnp.concatenate(
            [value_pool[b]] + [value_pool[slot(t)] for t in range(slots)] + [reg_value[...]], axis=1
        )

    def normalized(values, p):
        o = lax.dot_general(values, p, NN, preferred_element_type=jnp.float32)
        return o[:HEAD_SIZE] * (1.0 / o[HEAD_SIZE : HEAD_SIZE + 1])

    def output(i):
        b, lo, hi = steps[i]
        wide = (hi - lo) * rows
        values = gather_values(b, lambda t: table[b, t])
        o = normalized(values, weight_refs[i % 2][:, :wide])
        for c in range(lo, hi):
            out_ref[b * rows : (b + 1) * rows, c * HEAD_SIZE : (c + 1) * HEAD_SIZE] = (
                o[:, (c - lo) * rows : (c - lo + 1) * rows].T.astype(jnp.bfloat16)
            )

    count = len(steps)
    for i in range(count + 1):
        if i < count:
            weights(i)
        if i >= 1:
            output(i - 1)

    def exact(n, carry):
        b = n // GROUP
        at = pl.ds(pl.multiple_of(b * rows, rows), rows)
        cols = pl.ds(pl.multiple_of((n % GROUP) * HEAD_SIZE, HEAD_SIZE), HEAD_SIZE)

        def slot(t):
            entry = listed[b, t]
            return jnp.where(entry >= 0, blocks - 1 + ((entry // blocks) ^ me), fill)

        keys = jnp.concatenate(
            [key_pool[b]] + [key_pool[slot(t)] for t in range(slots)] + [reg_k[...]], axis=0
        )
        s = lax.dot_general(keys, q_ref[at, cols], NT, preferred_element_type=jnp.float32)
        s = jnp.concatenate([jnp.where(causal(b, rows), s[:rows], -jnp.inf), s[rows:]], axis=0)
        p = jnp.exp2((s - jnp.max(s, axis=0, keepdims=True)) * SCORE_SCALE).astype(jnp.bfloat16)
        out_ref[at, cols] = normalized(gather_values(b, slot), p).T.astype(jnp.bfloat16)
        return carry

    worst = over[0]
    for other in over[1:]:
        worst = jnp.maximum(worst, other)

    @pl.when(jnp.max(worst) * SCORE_SCALE > LARGEST_POWER)
    def _():
        lax.fori_loop(0, blocks * GROUP, exact, 0)


def attend(listed, image, me, q, own_k, own_v, mate_k, mate_v, arrived, regs, out, chunk):
    first, heads = chunk
    tokens = q.shape[0]
    blocks, slots = listed.shape
    rows = tokens // blocks
    reg = regs[0].shape[0]
    pool = blocks + 2 + 2 * len(arrived)
    keys = rows * (1 + slots) + reg
    smem = pl.BlockSpec(memory_space=pltpu.SMEM)

    def column(height):
        return pl.BlockSpec((height, HEAD_SIZE), lambda h: (0, first + h))

    wide = pl.BlockSpec((tokens, GROUP * HEAD_SIZE), lambda h: (0, first + h))
    block = pl.BlockSpec((2, 2, rows, HEAD_SIZE), lambda h: (0, 0, 0, h))
    operands = [listed, image, me, q, own_k, own_v, mate_k, mate_v, *arrived, *regs]
    hbm = pl.BlockSpec(memory_space=pltpu.HBM)
    specs = [smem] * 3 + [hbm] * 3 + [column(tokens)] * 2 + [block] * len(arrived) + [column(reg)] * 2
    aliases = {}
    if first > 0:
        aliases = {len(operands): 0}
        operands.append(out)
        specs.append(pl.BlockSpec(memory_space=pl.ANY))
    return pl.pallas_call(
        functools.partial(attend_kernel, first, len(arrived), slots, rows, reg),
        grid=(heads,),
        in_specs=specs,
        out_specs=wide,
        out_shape=jax.ShapeDtypeStruct(q.shape, jnp.bfloat16),
        scratch_shapes=[
            pltpu.VMEM((pool, rows, HEAD_SIZE), jnp.bfloat16),
            pltpu.VMEM((pool, HEAD_SIZE + ONES_ROWS, rows), jnp.bfloat16),
            pltpu.VMEM((HEAD_SIZE + ONES_ROWS, reg), jnp.bfloat16),
            pltpu.VMEM((keys, 2 * rows), jnp.bfloat16),
            pltpu.VMEM((keys, 2 * rows), jnp.bfloat16),
            pltpu.VMEM((2, tokens, GROUP * HEAD_SIZE), jnp.bfloat16),
            pltpu.VMEM((2, tokens, HEAD_SIZE), jnp.bfloat16),
            pltpu.VMEM((2, tokens, HEAD_SIZE), jnp.bfloat16),
            pltpu.SemaphoreType.DMA((3, 2)),
        ],
        input_output_aliases=aliases,
        compiler_params=pltpu.CompilerParams(vmem_limit_bytes=ATTEND_VMEM),
        cost_estimate=pl.CostEstimate(
            flops=4 * heads * GROUP * tokens * keys * HEAD_SIZE,
            bytes_accessed=4 * heads * GROUP * tokens * HEAD_SIZE,
            transcendentals=heads * GROUP * tokens * keys,
        ),
    )(*operands)


def layer(queries, keys, values, reg_owner, block_lists, list_counts, image_blocks):
    q = queries[0]
    own_k = keys[0]
    own_v = values[0]
    lists = block_lists[0]
    counts = list_counts[0]
    devices = lax.axis_size("seq")
    chips = devices // 2
    me = lax.axis_index("seq")
    blocks = lists.shape[0]
    slots = min(lists.shape[1], devices - 1)
    rows = own_k.shape[0] // blocks

    def swap(x, offset):
        return lax.ppermute(x, "seq", [(i, i ^ offset) for i in range(devices)])

    live = jnp.arange(slots, dtype=jnp.int32)[None, :] < counts[:, None]
    listed = jnp.where(live, lists[:, :slots], -1)
    tables = [swap(listed, 2 * d) for d in range(1, chips)]
    mate_k = swap(own_k, 1)
    mate_v = swap(own_v, 1)
    root = reg_owner[0]
    low = me % 2 == 0
    at_mate = (root ^ me) % 2 == 1
    half = jnp.where(
        low,
        jnp.where(at_mate, mate_k[:REG], own_k[:REG]),
        jnp.where(at_mate, mate_v[:REG], own_v[:REG]),
    )
    sends = select_blocks(
        me.reshape(1), tables, own_k, own_v, mate_k, mate_v, rows
    )
    arrived = [
        [swap(sends[piece * (chips - 1) + d - 1], 2 * d) for d in range(1, chips)]
        for piece in range(len(CHUNKS))
    ]
    found = half
    for d in range(1, chips):
        found = jnp.where((root ^ me) // 2 == d, swap(half, 2 * d), found)
    other = swap(found, 1)
    regs = (jnp.where(low, found, other), jnp.where(low, other, found))

    out = None
    for piece, chunk in enumerate(CHUNKS):
        out = attend(
            listed,
            image_blocks[0],
            me.reshape(1),
            q,
            own_k,
            own_v,
            mate_k,
            mate_v,
            arrived[piece],
            regs,
            out,
            chunk,
        )
    return out[None]


def solution(mesh):
    placed = (
        P("samp", "seq", None),
        P("samp", "seq", None),
        P("samp", "seq", None),
        P("samp"),
        P("samp", "seq", None),
        P("samp", "seq"),
        P("samp", "seq"),
    )
    return jax.shard_map(
        layer, mesh=mesh, in_specs=placed, out_specs=P("samp", "seq", None), check_vma=False
    )
```

```python
import functools
import math

import jax
import jax.numpy as jnp
from jax import lax
from jax.experimental import pallas as pl
from jax.experimental.pallas import tpu as pltpu
from jax.sharding import PartitionSpec as P


QUERY_HEADS = 28
KEY_VALUE_HEADS = 4
HEAD_SIZE = 128
REG = 64
GROUP = QUERY_HEADS // KEY_VALUE_HEADS
ONES_ROWS = 16
CHUNKS = ((0, 1), (1, 1), (2, 2))
SELECT_VMEM = int(56 * 2**20)
ATTEND_VMEM = 67043328
SCORE_SCALE = math.log2(math.e) / math.sqrt(HEAD_SIZE)
LARGEST_POWER = 64.0
NT = (((1,), (1,)), ((), ()))
NN = (((1,), (0,)), ((), ()))


def select_kernel(chips, rows, me_ref, *refs):
    tables = refs[: chips - 1]
    own_k, own_v, mate_k, mate_v = refs[chips - 1 : chips + 3]
    sends = refs[chips + 3 : -3]
    held, read_sem, write_sem = refs[-3:]
    me = me_ref[0]
    blocks = own_k.shape[0] // rows
    reads = []
    for chip in range(chips - 1):
        table = tables[chip]
        for side, (keys, values) in enumerate(((own_k, own_v), (mate_k, mate_v))):
            base = (me ^ side) * blocks
            block = jnp.int32(0)
            for b in range(table.shape[0]):
                for t in range(table.shape[1]):
                    place = table[b, t] - base
                    block = jnp.where((place >= 0) & (place < blocks), place, block)
            start = pl.multiple_of(block * rows, rows)
            for i, source in enumerate((keys, values)):
                copy = pltpu.make_async_copy(
                    source.at[pl.ds(start, rows)],
                    held.at[chip, side, i],
                    read_sem.at[chip, side, i],
                )
                copy.start()
                reads.append(copy)
    writes = []
    for chip in range(chips - 1):
        for copy in reads[4 * chip : 4 * chip + 4]:
            copy.wait()
        for piece, (first, count) in enumerate(CHUNKS):
            cols = pl.ds(first * HEAD_SIZE, count * HEAD_SIZE)
            copy = pltpu.make_async_copy(
                held.at[chip, :, :, :, cols],
                sends[piece * (chips - 1) + chip],
                write_sem.at[piece, chip],
            )
            copy.start()
            writes.append(copy)
    for copy in writes:
        copy.wait()


def select_blocks(me, tables, own_k, own_v, mate_k, mate_v, rows):
    chips = len(tables) + 1
    smem = pl.BlockSpec(memory_space=pltpu.SMEM)
    anywhere = pl.BlockSpec(memory_space=pl.ANY)
    shapes = [
        jax.ShapeDtypeStruct((2, 2, rows, count * HEAD_SIZE), jnp.bfloat16)
        for _, count in CHUNKS
        for _ in range(chips - 1)
    ]
    return pl.pallas_call(
        functools.partial(select_kernel, chips, rows),
        in_specs=[smem] * chips + [anywhere] * 4,
        out_specs=[anywhere] * len(shapes),
        out_shape=shapes,
        scratch_shapes=[
            pltpu.VMEM((chips - 1, 2, 2, rows, own_k.shape[1]), jnp.bfloat16),
            pltpu.SemaphoreType.DMA((chips - 1, 2, 2)),
            pltpu.SemaphoreType.DMA((len(CHUNKS), chips - 1)),
        ],
        compiler_params=pltpu.CompilerParams(vmem_limit_bytes=SELECT_VMEM),
        name="select_blocks",
    )(me, *tables, own_k, own_v, mate_k, mate_v)


def attend_kernel(first, heads, received, rows, listed, image, me_ref, *refs):
    q_ref, own_k, own_v, mate_k, mate_v = refs[:5]
    arrived = refs[5 : 5 + received]
    reg_k, reg_v = refs[5 + received : 7 + received]
    refs = refs[7 + received :]
    if first > 0:
        refs = refs[1:]
    out_ref = refs[0]
    key_pool, value_pool, reg_value, p0, p1, q_buf, k_buf, v_buf = refs[1:9]
    mate_buf, far_buf, reg_buf, o_buf, sem, write_sem = refs[9:]
    weight_refs = (p0, p1)
    tokens = k_buf.shape[0]
    blocks = tokens // rows
    slots = listed.shape[1]
    reg = reg_buf.shape[1]
    fill = key_pool.shape[1] - 1
    width = GROUP * HEAD_SIZE
    me = me_ref[0]
    table = {}
    from_mate = jnp.int32(0)
    for b in range(blocks):
        for t in range(slots):
            entry = listed[b, t]
            away = (entry // blocks) ^ me
            table[b, t] = jnp.where(entry >= 0, blocks - 1 + away, fill)
            from_mate = jnp.where((entry >= 0) & (away == 1), entry % blocks, from_mate)
    start = pl.multiple_of(from_mate * rows, rows)
    cols = pl.ds(first * HEAD_SIZE, heads * HEAD_SIZE)
    moves = [
        (q_ref.at[:, pl.ds((first + h) * width, width)], q_buf.at[h]) for h in range(heads)
    ]
    moves += [
        (own_k.at[:, cols], k_buf),
        (own_v.at[:, cols], v_buf),
        (mate_k.at[pl.ds(start, rows), cols], mate_buf.at[0]),
        (mate_v.at[pl.ds(start, rows), cols], mate_buf.at[1]),
        (reg_k.at[:, cols], reg_buf.at[0]),
        (reg_v.at[:, cols], reg_buf.at[1]),
    ]
    moves += [(arrived[d], far_buf.at[d]) for d in range(received)]
    copies = [pltpu.make_async_copy(x, y, sem.at[i]) for i, (x, y) in enumerate(moves)]
    for copy in copies:
        copy.start()
    row_ids = lax.broadcasted_iota(jnp.int32, (ONES_ROWS, rows), 0)
    ones = jnp.where(row_ids == 0, 1.0, 0.0).astype(jnp.bfloat16)
    for h in range(heads):
        for slot in range(fill):
            value_pool[h, slot, HEAD_SIZE:] = ones
        value_pool[h, fill] = jnp.zeros(value_pool.shape[2:], jnp.bfloat16)
        reg_value[h, HEAD_SIZE:] = ones[:, :reg]
    for copy in copies[heads:] + copies[:1]:
        copy.wait()

    def build(h):
        own = slice(h * HEAD_SIZE, (h + 1) * HEAD_SIZE)

        def put(slot, keys, values):
            key_pool[h, slot] = keys
            value_pool[h, slot, :HEAD_SIZE] = values.T

        for b in range(blocks):
            at = slice(b * rows, (b + 1) * rows)
            put(b, k_buf[at, own], v_buf[at, own])
        put(blocks, mate_buf[0, :, own], mate_buf[1, :, own])
        for d in range(received):
            for side in range(2):
                put(
                    blocks + 1 + 2 * d + side,
                    far_buf[d, side, 0, :, own],
                    far_buf[d, side, 1, :, own],
                )
        for r in range(rows // reg):
            key_pool[h, fill, r * reg : (r + 1) * reg] = reg_buf[0, :, own]
        reg_value[h, :HEAD_SIZE] = reg_buf[1, :, own].T

    def reg_keys(h):
        return key_pool[h, fill, :reg]

    def write(h, b):
        return pltpu.make_async_copy(
            o_buf.at[h, b],
            out_ref.at[pl.ds(b * rows, rows), pl.ds((first + h) * width, width)],
            write_sem.at[h, b],
        )

    steps = [
        (h, b, 2 * j, min(2 * j + 2, GROUP))
        for h in range(heads)
        for b in range(blocks)
        for j in range((GROUP + 1) // 2)
    ]
    over = []

    def causal(b, wide):
        key_row = lax.broadcasted_iota(jnp.int32, (rows, wide), 0)
        query_row = lax.broadcasted_iota(jnp.int32, (rows, wide), 1) % rows
        return (key_row <= query_row) | (image[b] == 1)

    def weights(i):
        h, b, lo, hi = steps[i]
        wide = (hi - lo) * rows
        p_ref = weight_refs[i % 2]
        q = jnp.concatenate(
            [
                q_buf[h, b * rows : (b + 1) * rows, c * HEAD_SIZE : (c + 1) * HEAD_SIZE]
                for c in range(lo, hi)
            ],
            axis=0,
        )
        near_keys = jnp.concatenate([key_pool[h, b], reg_keys(h)], axis=0)
        far_keys = jnp.concatenate([key_pool[h, table[b, t]] for t in range(slots)], axis=0)
        near = lax.dot_general(near_keys, q, NT, preferred_element_type=jnp.float32)
        far = lax.dot_general(far_keys, q, NT, preferred_element_type=jnp.float32)
        own = jnp.where(causal(b, wide), near[:rows], -jnp.inf)
        base = jnp.maximum(
            jnp.max(own, axis=0, keepdims=True), jnp.max(near[rows:], axis=0, keepdims=True)
        )
        top = jnp.max(far.reshape(-1, 8, wide), axis=0) - base
        over.append(jnp.maximum(top[:, :rows], top[:, wide - rows :]))

        def weigh(s):
            return jnp.exp2((s - base) * SCORE_SCALE).astype(jnp.bfloat16)

        p_ref[:rows, :wide] = weigh(own)
        p_ref[rows:-reg, :wide] = weigh(far)
        p_ref[-reg:, :wide] = weigh(near[rows:])

    def gather_values(h, b, slot):
        return jnp.concatenate(
            [value_pool[h, b]]
            + [value_pool[h, slot(t)] for t in range(slots)]
            + [reg_value[h]],
            axis=1,
        )

    def normalized(values, p):
        o = lax.dot_general(values, p, NN, preferred_element_type=jnp.float32)
        return o[:HEAD_SIZE] * (1.0 / o[HEAD_SIZE : HEAD_SIZE + 1])

    def output(i):
        h, b, lo, hi = steps[i]
        wide = (hi - lo) * rows
        values = gather_values(h, b, lambda t: table[b, t])
        o = normalized(values, weight_refs[i % 2][:, :wide])
        for c in range(lo, hi):
            o_buf[h, b, :, c * HEAD_SIZE : (c + 1) * HEAD_SIZE] = (
                o[:, (c - lo) * rows : (c - lo + 1) * rows].T.astype(jnp.bfloat16)
            )
        if hi == GROUP:
            write(h, b).start()

    build(0)
    count = len(steps)
    for i in range(count + 1):
        if i < count:
            if i > 0 and steps[i][0] != steps[i - 1][0]:
                copies[steps[i][0]].wait()
                build(steps[i][0])
            weights(i)
        if i >= 1:
            output(i - 1)
    for h in range(heads):
        for b in range(blocks):
            write(h, b).wait()

    worst = over[0]
    for other in over[1:]:
        worst = jnp.maximum(worst, other)

    @pl.when(jnp.max(worst) * SCORE_SCALE > LARGEST_POWER)
    def _():
        for h in range(heads):

            def exact(n, carry):
                b = n // GROUP
                at = pl.ds(pl.multiple_of(b * rows, rows), rows)
                lanes = pl.ds(pl.multiple_of((n % GROUP) * HEAD_SIZE, HEAD_SIZE), HEAD_SIZE)

                def slot(t):
                    entry = listed[b, t]
                    return jnp.where(entry >= 0, blocks - 1 + ((entry // blocks) ^ me), fill)

                keys = jnp.concatenate(
                    [key_pool[h, b]]
                    + [key_pool[h, slot(t)] for t in range(slots)]
                    + [reg_keys(h)],
                    axis=0,
                )
                s = lax.dot_general(
                    keys, q_buf[h, at, lanes], NT, preferred_element_type=jnp.float32
                )
                s = jnp.concatenate(
                    [jnp.where(causal(b, rows), s[:rows], -jnp.inf), s[rows:]], axis=0
                )
                p = jnp.exp2((s - jnp.max(s, axis=0, keepdims=True)) * SCORE_SCALE)
                o = normalized(gather_values(h, b, slot), p.astype(jnp.bfloat16))
                o_buf[h, b, :, lanes] = o.T.astype(jnp.bfloat16)
                return carry

            lax.fori_loop(0, blocks * GROUP, exact, 0)
            for b in range(blocks):
                write(h, b).start()
                write(h, b).wait()


def attend(listed, image, me, q, own_k, own_v, mate_k, mate_v, arrived, regs, out, chunk):
    first, heads = chunk
    tokens = q.shape[0]
    blocks, slots = listed.shape
    rows = tokens // blocks
    reg = regs[0].shape[0]
    pool = blocks + 2 + 2 * len(arrived)
    keys = rows * (1 + slots) + reg
    smem = pl.BlockSpec(memory_space=pltpu.SMEM)
    anywhere = pl.BlockSpec(memory_space=pl.ANY)
    operands = [listed, image, me, q, own_k, own_v, mate_k, mate_v, *arrived, *regs]
    aliases = {}
    if first > 0:
        aliases = {len(operands): 0}
        operands.append(out)
    bf16 = jnp.bfloat16
    cols = heads * HEAD_SIZE
    return pl.pallas_call(
        functools.partial(attend_kernel, first, heads, len(arrived), rows),
        in_specs=[smem] * 3 + [anywhere] * (len(operands) - 3),
        out_specs=anywhere,
        out_shape=jax.ShapeDtypeStruct(q.shape, bf16),
        scratch_shapes=[
            pltpu.VMEM((heads, pool, rows, HEAD_SIZE), bf16),
            pltpu.VMEM((heads, pool, HEAD_SIZE + ONES_ROWS, rows), bf16),
            pltpu.VMEM((heads, HEAD_SIZE + ONES_ROWS, reg), bf16),
            pltpu.VMEM((keys, 2 * rows), bf16),
            pltpu.VMEM((keys, 2 * rows), bf16),
            pltpu.VMEM((heads, tokens, GROUP * HEAD_SIZE), bf16),
            pltpu.VMEM((tokens, cols), bf16),
            pltpu.VMEM((tokens, cols), bf16),
            pltpu.VMEM((2, rows, cols), bf16),
            pltpu.VMEM((len(arrived), 2, 2, rows, cols), bf16),
            pltpu.VMEM((2, reg, cols), bf16),
            pltpu.VMEM((heads, blocks, rows, GROUP * HEAD_SIZE), bf16),
            pltpu.SemaphoreType.DMA((heads + 6 + len(arrived),)),
            pltpu.SemaphoreType.DMA((heads, blocks)),
        ],
        input_output_aliases=aliases,
        compiler_params=pltpu.CompilerParams(vmem_limit_bytes=ATTEND_VMEM),
        cost_estimate=pl.CostEstimate(
            flops=4 * heads * GROUP * tokens * keys * HEAD_SIZE,
            bytes_accessed=4 * heads * GROUP * tokens * HEAD_SIZE,
            transcendentals=heads * GROUP * tokens * keys,
        ),
    )(*operands)


def layer(queries, keys, values, reg_owner, block_lists, list_counts, image_blocks):
    q = queries[0]
    own_k = keys[0]
    own_v = values[0]
    lists = block_lists[0]
    counts = list_counts[0]
    devices = lax.axis_size("seq")
    chips = devices // 2
    me = lax.axis_index("seq")
    blocks = lists.shape[0]
    slots = min(lists.shape[1], devices - 1)
    rows = own_k.shape[0] // blocks

    def swap(x, offset):
        return lax.ppermute(x, "seq", [(i, i ^ offset) for i in range(devices)])

    live = jnp.arange(slots, dtype=jnp.int32)[None, :] < counts[:, None]
    listed = jnp.where(live, lists[:, :slots], -1)
    tables = [swap(listed, 2 * d) for d in range(1, chips)]
    mate_k = swap(own_k, 1)
    mate_v = swap(own_v, 1)
    root = reg_owner[0]
    low = me % 2 == 0
    at_mate = (root ^ me) % 2 == 1
    half = jnp.where(
        low,
        jnp.where(at_mate, mate_k[:REG], own_k[:REG]),
        jnp.where(at_mate, mate_v[:REG], own_v[:REG]),
    )
    sends = select_blocks(
        me.reshape(1), tables, own_k, own_v, mate_k, mate_v, rows
    )
    arrived = [
        [swap(sends[piece * (chips - 1) + d - 1], 2 * d) for d in range(1, chips)]
        for piece in range(len(CHUNKS))
    ]
    found = half
    for d in range(1, chips):
        found = jnp.where((root ^ me) // 2 == d, swap(half, 2 * d), found)
    other = swap(found, 1)
    regs = (jnp.where(low, found, other), jnp.where(low, other, found))

    out = None
    for piece, chunk in enumerate(CHUNKS):
        out = attend(
            listed,
            image_blocks[0],
            me.reshape(1),
            q,
            own_k,
            own_v,
            mate_k,
            mate_v,
            arrived[piece],
            regs,
            out,
            chunk,
        )
    return out[None]


def solution(mesh):
    placed = (
        P("samp", "seq", None),
        P("samp", "seq", None),
        P("samp", "seq", None),
        P("samp"),
        P("samp", "seq", None),
        P("samp", "seq"),
        P("samp", "seq"),
    )
    return jax.shard_map(
        layer, mesh=mesh, in_specs=placed, out_specs=P("samp", "seq", None), check_vma=False
    )
```

```python
import functools
import math

import jax
import jax.numpy as jnp
from jax import lax
from jax.experimental import pallas as pl
from jax.experimental.pallas import tpu as pltpu
from jax.sharding import PartitionSpec as P


QUERY_HEADS = 28
KEY_VALUE_HEADS = 4
HEAD_SIZE = 128
REG = 64
GROUP = QUERY_HEADS // KEY_VALUE_HEADS
ONES_ROWS = 16
CHUNKS = ((0, 1), (1, 1), (2, 2))
SELECT_VMEM = int(56 * 2**20)
ATTEND_VMEM = 67043328
SCORE_SCALE = math.log2(math.e) / math.sqrt(HEAD_SIZE)
LARGEST_POWER = 64.0
NT = (((1,), (1,)), ((), ()))
NN = (((1,), (0,)), ((), ()))


def select_kernel(chips, rows, me_ref, *refs):
    tables = refs[: chips - 1]
    own_k, own_v, mate_k, mate_v = refs[chips - 1 : chips + 3]
    sends = refs[chips + 3 : -3]
    held, read_sem, write_sem = refs[-3:]
    me = me_ref[0]
    blocks = own_k.shape[0] // rows
    reads = []
    for chip in range(chips - 1):
        table = tables[chip]
        for side, (keys, values) in enumerate(((own_k, own_v), (mate_k, mate_v))):
            base = (me ^ side) * blocks
            block = jnp.int32(0)
            for b in range(table.shape[0]):
                for t in range(table.shape[1]):
                    place = table[b, t] - base
                    block = jnp.where((place >= 0) & (place < blocks), place, block)
            start = pl.multiple_of(block * rows, rows)
            for i, source in enumerate((keys, values)):
                copy = pltpu.make_async_copy(
                    source.at[pl.ds(start, rows)],
                    held.at[chip, side, i],
                    read_sem.at[chip, side, i],
                )
                copy.start()
                reads.append(copy)
    writes = []
    for chip in range(chips - 1):
        for copy in reads[4 * chip : 4 * chip + 4]:
            copy.wait()
        for piece, (first, count) in enumerate(CHUNKS):
            cols = pl.ds(first * HEAD_SIZE, count * HEAD_SIZE)
            copy = pltpu.make_async_copy(
                held.at[chip, :, :, :, cols],
                sends[piece * (chips - 1) + chip],
                write_sem.at[piece, chip],
            )
            copy.start()
            writes.append(copy)
    for copy in writes:
        copy.wait()


def select_blocks(me, tables, own_k, own_v, mate_k, mate_v, rows):
    chips = len(tables) + 1
    smem = pl.BlockSpec(memory_space=pltpu.SMEM)
    anywhere = pl.BlockSpec(memory_space=pl.ANY)
    shapes = [
        jax.ShapeDtypeStruct((2, 2, rows, count * HEAD_SIZE), jnp.bfloat16)
        for _, count in CHUNKS
        for _ in range(chips - 1)
    ]
    return pl.pallas_call(
        functools.partial(select_kernel, chips, rows),
        in_specs=[smem] * chips + [anywhere] * 4,
        out_specs=[anywhere] * len(shapes),
        out_shape=shapes,
        scratch_shapes=[
            pltpu.VMEM((chips - 1, 2, 2, rows, own_k.shape[1]), jnp.bfloat16),
            pltpu.SemaphoreType.DMA((chips - 1, 2, 2)),
            pltpu.SemaphoreType.DMA((len(CHUNKS), chips - 1)),
        ],
        compiler_params=pltpu.CompilerParams(vmem_limit_bytes=SELECT_VMEM),
        name="select_blocks",
    )(me, *tables, own_k, own_v, mate_k, mate_v)


def attend_kernel(first, heads, received, rows, listed, image, me_ref, *refs):
    q_ref, own_k, own_v, mate_k, mate_v = refs[:5]
    arrived = refs[5 : 5 + received]
    reg_k, reg_v = refs[5 + received : 7 + received]
    refs = refs[7 + received :]
    if first > 0:
        refs = refs[1:]
    out_ref = refs[0]
    key_pool, value_pool, reg_value, p0, p1, q_buf, k_buf, v_buf = refs[1:9]
    mate_buf, far_buf, reg_buf, o_buf, sem, write_sem = refs[9:]
    weight_refs = (p0, p1)
    tokens = k_buf.shape[0]
    blocks = tokens // rows
    slots = listed.shape[1]
    reg = reg_buf.shape[1]
    fill = key_pool.shape[1] - 1
    width = GROUP * HEAD_SIZE
    me = me_ref[0]
    cols = pl.ds(first * HEAD_SIZE, heads * HEAD_SIZE)
    moves = [
        (q_ref.at[:, pl.ds((first + h) * width, width)], q_buf.at[h]) for h in range(heads)
    ]
    moves += [
        (own_k.at[:, cols], k_buf),
        (own_v.at[:, cols], v_buf),
        (reg_k.at[:, cols], reg_buf.at[0]),
        (reg_v.at[:, cols], reg_buf.at[1]),
    ]
    moves += [(arrived[d], far_buf.at[d]) for d in range(received)]
    copies = [pltpu.make_async_copy(x, y, sem.at[i]) for i, (x, y) in enumerate(moves)]
    for copy in copies[heads:] + copies[:heads]:
        copy.start()
    table = {}
    from_mate = jnp.int32(0)
    for b in range(blocks):
        for t in range(slots):
            entry = listed[b, t]
            away = (entry // blocks) ^ me
            table[b, t] = jnp.where(entry >= 0, blocks - 1 + away, fill)
            from_mate = jnp.where((entry >= 0) & (away == 1), entry % blocks, from_mate)
    start = pl.multiple_of(from_mate * rows, rows)
    for i, source in enumerate((mate_k, mate_v)):
        copy = pltpu.make_async_copy(
            source.at[pl.ds(start, rows), cols], mate_buf.at[i], sem.at[len(copies)]
        )
        copy.start()
        copies.append(copy)
    row_ids = lax.broadcasted_iota(jnp.int32, (ONES_ROWS, rows), 0)
    ones = jnp.where(row_ids == 0, 1.0, 0.0).astype(jnp.bfloat16)
    for h in range(heads):
        for slot in range(fill):
            value_pool[h, slot, HEAD_SIZE:] = ones
        value_pool[h, fill] = jnp.zeros(value_pool.shape[2:], jnp.bfloat16)
        reg_value[h, HEAD_SIZE:] = ones[:, :reg]
    for copy in copies[heads:] + copies[:1]:
        copy.wait()

    def build(h):
        own = slice(h * HEAD_SIZE, (h + 1) * HEAD_SIZE)

        def put(slot, keys, values):
            key_pool[h, slot] = keys
            value_pool[h, slot, :HEAD_SIZE] = values.T

        for b in range(blocks):
            at = slice(b * rows, (b + 1) * rows)
            put(b, k_buf[at, own], v_buf[at, own])
        put(blocks, mate_buf[0, :, own], mate_buf[1, :, own])
        for d in range(received):
            for side in range(2):
                put(
                    blocks + 1 + 2 * d + side,
                    far_buf[d, side, 0, :, own],
                    far_buf[d, side, 1, :, own],
                )
        for r in range(rows // reg):
            key_pool[h, fill, r * reg : (r + 1) * reg] = reg_buf[0, :, own]
        reg_value[h, :HEAD_SIZE] = reg_buf[1, :, own].T

    def reg_keys(h):
        return key_pool[h, fill, :reg]

    def write(h, b):
        return pltpu.make_async_copy(
            o_buf.at[h, b],
            out_ref.at[pl.ds(b * rows, rows), pl.ds((first + h) * width, width)],
            write_sem.at[h, b],
        )

    steps = [
        (h, b, 2 * j, min(2 * j + 2, GROUP))
        for h in range(heads)
        for b in range(blocks)
        for j in range((GROUP + 1) // 2)
    ]
    over = []

    def causal(b, wide):
        key_row = lax.broadcasted_iota(jnp.int32, (rows, wide), 0)
        query_row = lax.broadcasted_iota(jnp.int32, (rows, wide), 1) % rows
        return (key_row <= query_row) | (image[b] == 1)

    def weights(i):
        h, b, lo, hi = steps[i]
        wide = (hi - lo) * rows
        p_ref = weight_refs[i % 2]
        q = jnp.concatenate(
            [
                q_buf[h, b * rows : (b + 1) * rows, c * HEAD_SIZE : (c + 1) * HEAD_SIZE]
                for c in range(lo, hi)
            ],
            axis=0,
        )
        near_keys = jnp.concatenate([key_pool[h, b], reg_keys(h)], axis=0)
        far_keys = jnp.concatenate([key_pool[h, table[b, t]] for t in range(slots)], axis=0)
        near = lax.dot_general(near_keys, q, NT, preferred_element_type=jnp.float32)
        far = lax.dot_general(far_keys, q, NT, preferred_element_type=jnp.float32)
        own = jnp.where(causal(b, wide), near[:rows], -jnp.inf)
        base = jnp.maximum(
            jnp.max(own, axis=0, keepdims=True), jnp.max(near[rows:], axis=0, keepdims=True)
        )
        top = jnp.max(far.reshape(-1, 8, wide), axis=0) - base
        over.append(jnp.maximum(top[:, :rows], top[:, wide - rows :]))

        def weigh(s):
            return jnp.exp2((s - base) * SCORE_SCALE).astype(jnp.bfloat16)

        p_ref[:rows, :wide] = weigh(own)
        p_ref[rows:-reg, :wide] = weigh(far)
        p_ref[-reg:, :wide] = weigh(near[rows:])

    def gather_values(h, b, slot):
        return jnp.concatenate(
            [value_pool[h, b]]
            + [value_pool[h, slot(t)] for t in range(slots)]
            + [reg_value[h]],
            axis=1,
        )

    def normalized(values, p):
        o = lax.dot_general(values, p, NN, preferred_element_type=jnp.float32)
        return o[:HEAD_SIZE] * (1.0 / o[HEAD_SIZE : HEAD_SIZE + 1])

    def output(i):
        h, b, lo, hi = steps[i]
        wide = (hi - lo) * rows
        values = gather_values(h, b, lambda t: table[b, t])
        o = normalized(values, weight_refs[i % 2][:, :wide])
        for c in range(lo, hi):
            o_buf[h, b, :, c * HEAD_SIZE : (c + 1) * HEAD_SIZE] = (
                o[:, (c - lo) * rows : (c - lo + 1) * rows].T.astype(jnp.bfloat16)
            )
        if hi == GROUP:
            write(h, b).start()

    build(0)
    count = len(steps)
    for i in range(count + 1):
        if i < count:
            if i > 0 and steps[i][0] != steps[i - 1][0]:
                copies[steps[i][0]].wait()
                build(steps[i][0])
            weights(i)
        if i >= 1:
            output(i - 1)
    worst = over[0]
    for other in over[1:]:
        worst = jnp.maximum(worst, other)

    unsafe = jnp.max(worst) * SCORE_SCALE > LARGEST_POWER
    for h in range(heads):
        for b in range(blocks):
            write(h, b).wait()

    @pl.when(unsafe)
    def _():
        for h in range(heads):

            def exact(n, carry):
                b = n // GROUP
                at = pl.ds(pl.multiple_of(b * rows, rows), rows)
                lanes = pl.ds(pl.multiple_of((n % GROUP) * HEAD_SIZE, HEAD_SIZE), HEAD_SIZE)

                def slot(t):
                    entry = listed[b, t]
                    return jnp.where(entry >= 0, blocks - 1 + ((entry // blocks) ^ me), fill)

                keys = jnp.concatenate(
                    [key_pool[h, b]]
                    + [key_pool[h, slot(t)] for t in range(slots)]
                    + [reg_keys(h)],
                    axis=0,
                )
                s = lax.dot_general(
                    keys, q_buf[h, at, lanes], NT, preferred_element_type=jnp.float32
                )
                s = jnp.concatenate(
                    [jnp.where(causal(b, rows), s[:rows], -jnp.inf), s[rows:]], axis=0
                )
                p = jnp.exp2((s - jnp.max(s, axis=0, keepdims=True)) * SCORE_SCALE)
                o = normalized(gather_values(h, b, slot), p.astype(jnp.bfloat16))
                o_buf[h, b, :, lanes] = o.T.astype(jnp.bfloat16)
                return carry

            lax.fori_loop(0, blocks * GROUP, exact, 0)
            for b in range(blocks):
                write(h, b).start()
                write(h, b).wait()


def attend(listed, image, me, q, own_k, own_v, mate_k, mate_v, arrived, regs, out, chunk):
    first, heads = chunk
    tokens = q.shape[0]
    blocks, slots = listed.shape
    rows = tokens // blocks
    reg = regs[0].shape[0]
    pool = blocks + 2 + 2 * len(arrived)
    keys = rows * (1 + slots) + reg
    smem = pl.BlockSpec(memory_space=pltpu.SMEM)
    anywhere = pl.BlockSpec(memory_space=pl.ANY)
    operands = [listed, image, me, q, own_k, own_v, mate_k, mate_v, *arrived, *regs]
    aliases = {}
    if first > 0:
        aliases = {len(operands): 0}
        operands.append(out)
    bf16 = jnp.bfloat16
    cols = heads * HEAD_SIZE
    return pl.pallas_call(
        functools.partial(attend_kernel, first, heads, len(arrived), rows),
        in_specs=[smem] * 3 + [anywhere] * (len(operands) - 3),
        out_specs=anywhere,
        out_shape=jax.ShapeDtypeStruct(q.shape, bf16),
        scratch_shapes=[
            pltpu.VMEM((heads, pool, rows, HEAD_SIZE), bf16),
            pltpu.VMEM((heads, pool, HEAD_SIZE + ONES_ROWS, rows), bf16),
            pltpu.VMEM((heads, HEAD_SIZE + ONES_ROWS, reg), bf16),
            pltpu.VMEM((keys, 2 * rows), bf16),
            pltpu.VMEM((keys, 2 * rows), bf16),
            pltpu.VMEM((heads, tokens, GROUP * HEAD_SIZE), bf16),
            pltpu.VMEM((tokens, cols), bf16),
            pltpu.VMEM((tokens, cols), bf16),
            pltpu.VMEM((2, rows, cols), bf16),
            pltpu.VMEM((len(arrived), 2, 2, rows, cols), bf16),
            pltpu.VMEM((2, reg, cols), bf16),
            pltpu.VMEM((heads, blocks, rows, GROUP * HEAD_SIZE), bf16),
            pltpu.SemaphoreType.DMA((heads + 6 + len(arrived),)),
            pltpu.SemaphoreType.DMA((heads, blocks)),
        ],
        input_output_aliases=aliases,
        compiler_params=pltpu.CompilerParams(vmem_limit_bytes=ATTEND_VMEM),
        cost_estimate=pl.CostEstimate(
            flops=4 * heads * GROUP * tokens * keys * HEAD_SIZE,
            bytes_accessed=4 * heads * GROUP * tokens * HEAD_SIZE,
            transcendentals=heads * GROUP * tokens * keys,
        ),
    )(*operands)


def layer(queries, keys, values, reg_owner, block_lists, list_counts, image_blocks):
    q = queries[0]
    own_k = keys[0]
    own_v = values[0]
    lists = block_lists[0]
    counts = list_counts[0]
    devices = lax.axis_size("seq")
    chips = devices // 2
    me = lax.axis_index("seq")
    blocks = lists.shape[0]
    slots = min(lists.shape[1], devices - 1)
    rows = own_k.shape[0] // blocks

    def swap(x, offset):
        return lax.ppermute(x, "seq", [(i, i ^ offset) for i in range(devices)])

    live = jnp.arange(slots, dtype=jnp.int32)[None, :] < counts[:, None]
    listed = jnp.where(live, lists[:, :slots], -1)
    tables = [swap(listed, 2 * d) for d in range(1, chips)]
    mate_k = swap(own_k, 1)
    mate_v = swap(own_v, 1)
    root = reg_owner[0]
    low = me % 2 == 0
    at_mate = (root ^ me) % 2 == 1
    half = jnp.where(
        low,
        jnp.where(at_mate, mate_k[:REG], own_k[:REG]),
        jnp.where(at_mate, mate_v[:REG], own_v[:REG]),
    )
    sends = select_blocks(
        me.reshape(1), tables, own_k, own_v, mate_k, mate_v, rows
    )
    arrived = [
        [swap(sends[piece * (chips - 1) + d - 1], 2 * d) for d in range(1, chips)]
        for piece in range(len(CHUNKS))
    ]
    found = half
    for d in range(1, chips):
        found = jnp.where((root ^ me) // 2 == d, swap(half, 2 * d), found)
    other = swap(found, 1)
    regs = (jnp.where(low, found, other), jnp.where(low, other, found))

    out = None
    for piece, chunk in enumerate(CHUNKS):
        out = attend(
            listed,
            image_blocks[0],
            me.reshape(1),
            q,
            own_k,
            own_v,
            mate_k,
            mate_v,
            arrived[piece],
            regs,
            out,
            chunk,
        )
    return out[None]


def solution(mesh):
    placed = (
        P("samp", "seq", None),
        P("samp", "seq", None),
        P("samp", "seq", None),
        P("samp"),
        P("samp", "seq", None),
        P("samp", "seq"),
        P("samp", "seq"),
    )
    return jax.shard_map(
        layer, mesh=mesh, in_specs=placed, out_specs=P("samp", "seq", None), check_vma=False
    )
```
